128 devices in a mesh: rows: 32 (over y, z, core), tgt: 4 (over x).
Axes of the slice: x: 4, y: 4, z: 4, core: 2. Of those that a mesh axis runs over, the one named last changes fastest.
Arguments:
- frames: bfloat16 [65536, 512], P('rows', 'tgt'), may hold values from -6 to 6
- weights: bfloat16 [512, 1024], replicated, may hold values from -0.25 to 0.25
- phases: float32 [1024], replicated, may hold values from -3.140625 to 3.140625
- residual: float32 [65536, 1024], P('rows', 'tgt'), may hold values from -6 to 6
Outputs:
- residual_next: float32 [65536, 1024], P('rows', 'tgt')
- coefficients: float32 [1024, 1024], P(None, 'tgt')
The draws below stay inside these ranges and needn't reach their ends.
All inputs are finite; a program needn't handle non-finite values.
Results may differ from the reference program's by a relative error of at most 0.0003.
Values may be sent and summed in bfloat16 or wider, within the bound.
No kernel may reach another device: no remote copies, remote signals or barrier semaphores. Data moves between devices by JAX's collectives and lax.ppermute only.
A program may use at most 128 MiB of HBM per device.

```python
import jax
import jax.numpy as jnp
from jax import lax

DIN = 512
FEAT = 1024
TGT = 1024
TOTAL = 65536


def block_levels(own_key, extent, shards, smallest, top_value):
    def one(axis_at, blocks):
        steps = jax.random.uniform(jax.random.fold_in(jax.random.fold_in(own_key, 6), axis_at), (blocks,), jnp.float32, smallest / len(shards), top_value / len(shards))
        return jnp.repeat(jnp.exp(steps), extent[axis_at] // blocks).reshape((-1,) + (1,) * (len(extent) - axis_at - 1))

    level = one(*shards[0])
    for cut in shards[1:]:
        level = level * one(*cut)
    return level


def noise(rng, dims, spread, most, split=(), kind=jnp.bfloat16):
    result = jax.random.normal(rng, dims, jnp.float32) * spread
    if len(split) > 0:
        result = block_levels(rng, dims, split, -0.22, 0.18) * result
    return jnp.clip(result, min=-most, max=most).astype(kind)


def setup_inputs(seed: int = 0) -> dict:
    arg_keys = jax.random.split(jax.random.key(seed), 5)
    return {
        "frames": noise(arg_keys[0], (TOTAL, DIN), 1.0, 6.0, ((0, 32), (1, 4))),
        "weights": noise(arg_keys[1], (DIN, FEAT), DIN ** -0.5, 0.25),
        "phases": jnp.clip(jax.random.uniform(arg_keys[2], (FEAT,), jnp.float32, -3.140625, 3.140625), -3.140625, 3.140625),
        "residual": noise(arg_keys[3], (TOTAL, TGT), 1.0, 6.0, ((0, 32), (1, 4)), jnp.float32),
    }


def reference(frames, weights, phases, residual):
    highest = lax.Precision.HIGHEST
    preact = jnp.dot(frames.astype(jnp.float32), weights.astype(jnp.float32), preferred_element_type=jnp.float32)
    feature = jnp.sqrt(2.0 / FEAT) * jnp.cos(preact + phases[None, :])
    gram_matrix = jnp.dot(feature.T.astype(jnp.float32), feature.astype(jnp.float32), precision=highest, preferred_element_type=jnp.float32)
    gram_matrix = gram_matrix + 0.1 * TOTAL / FEAT * jnp.eye(FEAT, dtype=jnp.float32)
    correlation = jnp.dot(feature.T.astype(jnp.float32), residual.astype(jnp.float32), precision=highest, preferred_element_type=jnp.float32)
    factor = jnp.linalg.cholesky(gram_matrix)
    coefficients = jax.scipy.linalg.cho_solve((factor, True), correlation)
    residual_next = residual - jnp.dot(feature.astype(jnp.float32), coefficients.astype(jnp.float32), precision=highest, preferred_element_type=jnp.float32)
    return (residual_next, coefficients)
```

```python
import math

import jax
import jax.numpy as jnp
from jax import lax
from jax.experimental import pallas as pl
from jax.experimental.pallas import tpu as pltpu
from jax.sharding import PartitionSpec as P

F32 = jnp.float32
BF16 = jnp.bfloat16
HIGHEST = lax.Precision.HIGHEST
NB = 128
PB = 16
SIN_PI = (
    3.1415926535362892,
    -5.167712764624528,
    2.5501633189472983,
    -0.5992521978285216,
    0.08205040183240117,
    -0.007028386446239114,
)


def dot(a, b, precision=None):
    return lax.dot_general(
        a, b, (((1,), (0,)), ((), ())), precision=precision, preferred_element_type=F32
    )


def dot_t(a, b, precision=None):
    return lax.dot_general(
        a, b, (((0,), (0,)), ((), ())), precision=precision, preferred_element_type=F32
    )


def split2(x):
    high = x.astype(BF16)
    return high, (x - high.astype(F32)).astype(BF16)


def split3(x):
    high = x.astype(BF16)
    rest = x - high.astype(F32)
    mid = rest.astype(BF16)
    return high, mid, (rest - mid.astype(F32)).astype(BF16)


def features(frames, weights, phases):
    turns = (dot(frames, weights) + phases) * (0.5 / math.pi)
    r = turns - jnp.round(turns)
    s = r * r
    poly = jnp.full_like(s, SIN_PI[-1])
    for coef in SIN_PI[-2::-1]:
        poly = poly * s + coef
    half = poly * r
    scale = math.sqrt(2.0 / weights.shape[1])
    return scale - (2.0 * scale) * (half * half)


def packed_slot(block, blocks):
    if block < blocks // 2:
        return block, 0
    return blocks - 1 - block, (block + 1) * NB


def gram_kernel(frames, weights, phases, out, high, low):
    blocks = out.shape[0] * 2
    h, l = split2(features(frames[...], weights[...], phases[...]))
    high[...] = h
    low[...] = l
    for i in range(blocks):
        rows = slice(i * NB, (i + 1) * NB)
        right = slice(i * NB, blocks * NB)
        g = dot_t(high[:, rows], high[:, right])
        g = g + dot_t(high[:, rows], low[:, right])
        g = g + dot_t(low[:, rows], high[:, right])
        at, col = packed_slot(i, blocks)
        out[at, :, col : col + (blocks - i) * NB] = g


def feature_kernel(frames, weights, phases, residual, high, low, corr):
    h, l = split2(features(frames[...], weights[...], phases[...]))
    high[...] = h
    low[...] = l
    rh, rl = split2(residual[...])
    part = dot_t(h, rh) + dot_t(h, rl) + dot_t(l, rh)

    @pl.when(pl.program_id(0) == 0)
    def _():
        corr[...] = part

    @pl.when(pl.program_id(0) > 0)
    def _():
        corr[...] += part


def invert_block(d):
    lane = lax.broadcasted_iota(jnp.int32, (PB, NB), 1)
    sub = lax.broadcasted_iota(jnp.int32, (PB, NB), 0)
    col_at = lax.broadcasted_iota(jnp.int32, (NB, NB), 1)
    zero = jnp.zeros((PB, NB), F32)
    for k0 in range(0, NB, PB):
        rows = d[k0 : k0 + PB, :]
        cols = [jnp.broadcast_to(rows[:, k0 + j : k0 + j + 1], (PB, NB)) for j in range(PB)]
        lh, lm, ll = split3(jnp.where(lane < k0, -rows, rows))
        left = jnp.concatenate([lh, lh, lm, lm, lh, ll], axis=0)
        x = jnp.where((lane >= k0) & (lane < k0 + PB), jnp.where(lane - k0 == sub, 1.0, 0.0), rows)
        scale = zero
        for k in range(PB):
            c = cols[k]
            p = 1.0 / c[k : k + 1, :]
            m = jnp.where(sub == k, 0.0, c * p)
            scale = jnp.where(sub == k, p, scale)
            for j in range(k + 1, PB):
                cols[j] = cols[j] - m * cols[j][k : k + 1, :]
            x = x - m * x[k : k + 1, :]
        x = x * scale
        xh, xm, xl = split3(x)
        right = jnp.concatenate([xh, xm, xh, xm, xl, xh], axis=0)
        update = dot_t(left, right)
        kept = d[...]
        d[...] = jnp.where((col_at >= k0) & (col_at < k0 + PB), 0.0, kept) - update
        d[k0 : k0 + PB, :] = x


def factor_kernel(pack, panel, inverse, a, d, *, ridge):
    blocks = panel.shape[0]
    size = blocks * NB
    for i in range(blocks):
        at, col = packed_slot(i, blocks)
        a[i, :, i * NB : size] = pack[at, :, col : col + size - i * NB]
        if i > 0:
            a[i, :, : i * NB] = jnp.zeros((NB, i * NB), F32)
            panel[i, :, : i * NB] = jnp.zeros((NB, i * NB), F32)
    eye = jnp.where(
        lax.broadcasted_iota(jnp.int32, (NB, NB), 0) == lax.broadcasted_iota(jnp.int32, (NB, NB), 1),
        ridge,
        0.0,
    ).astype(F32)

    def step(i, _):
        own = pl.ds(pl.multiple_of(i * NB, NB), NB)
        d[...] = a[i, :, own] + eye
        invert_block(d)
        inverse[i] = d[...]

        def eliminate(first):
            panel[i, :, first:] = dot(d[...], a[i, :, first:], HIGHEST)

            def row(j, _):
                left = a[i, :, pl.ds(pl.multiple_of(j * NB, NB), NB)]
                a[j, :, first:] = a[j, :, first:] - dot_t(left, panel[i, :, first:], HIGHEST)
                return 0

            lax.fori_loop(i + 1, blocks, row, 0)

        for part in range(4):
            low = part * (blocks // 4)

            @pl.when((i >= low) & (i < low + blocks // 4))
            def _():
                eliminate(low * NB)

        return 0

    lax.fori_loop(0, blocks, step, 0)


def solve_kernel(panel, inverse, corr, out, c):
    blocks = panel.shape[0]
    c[...] = jnp.zeros_like(c)
    for i in range(blocks):
        rows = slice(i * NB, (i + 1) * NB)
        value = corr[rows, :]
        for j in range(i):
            value = value - dot_t(panel[j, :, rows], c[j * NB : (j + 1) * NB, :], HIGHEST)
        c[rows, :] = value
    for i in range(blocks - 1, -1, -1):
        rows = slice(i * NB, (i + 1) * NB)
        value = dot(inverse[i], c[rows, :], HIGHEST)
        if i < blocks - 1:
            rest = (i + 1) * NB
            value = value - dot(panel[i, :, rest:], out[rest:, :], HIGHEST)
        out[rows, :] = value


def update_kernel(high, low, coef, residual, out):
    wh, wl = split2(coef[...])
    h = high[...]
    out[...] = residual[...] - (dot(h, wh) + dot(h, wl) + dot(low[...], wh))


def params(**kw):
    return pltpu.CompilerParams(vmem_limit_bytes=56 * 1024 * 1024, **kw)


def factor_call(pack, ridge):
    blocks = pack.shape[0] * 2
    return pl.pallas_call(
        lambda *refs: factor_kernel(*refs, ridge=ridge),
        out_shape=(
            jax.ShapeDtypeStruct((blocks, NB, blocks * NB), F32),
            jax.ShapeDtypeStruct((blocks, NB, NB), F32),
        ),
        scratch_shapes=[
            pltpu.VMEM((blocks, NB, blocks * NB), F32),
            pltpu.VMEM((NB, NB), F32),
        ],
        compiler_params=params(),
        name="factor",
    )(pack)


def solve_call(panel, inverse, corr):
    return pl.pallas_call(
        solve_kernel,
        out_shape=jax.ShapeDtypeStruct(corr.shape, F32),
        scratch_shapes=[pltpu.VMEM(corr.shape, F32)],
        compiler_params=params(),
        name="solve",
    )(panel, inverse, corr)


def gram_call(frames, weights, phases):
    rows = frames.shape[0]
    feat = weights.shape[1]
    blocks = feat // NB
    return pl.pallas_call(
        gram_kernel,
        out_shape=jax.ShapeDtypeStruct((blocks // 2, NB, feat + NB), F32),
        scratch_shapes=[pltpu.VMEM((rows, feat), BF16), pltpu.VMEM((rows, feat), BF16)],
        compiler_params=params(),
        name="gram",
    )(frames, weights, phases)


def feature_call(frames, weights, phases, residual, tile=256):
    rows, din = frames.shape
    feat = weights.shape[1]
    cols = residual.shape[1]
    return pl.pallas_call(
        feature_kernel,
        grid=(rows // tile,),
        in_specs=[
            pl.BlockSpec((tile, din), lambda i: (i, 0)),
            pl.BlockSpec((din, feat), lambda i: (0, 0)),
            pl.BlockSpec((1, feat), lambda i: (0, 0)),
            pl.BlockSpec((tile, cols), lambda i: (i, 0)),
        ],
        out_specs=[
            pl.BlockSpec((tile, feat), lambda i: (i, 0)),
            pl.BlockSpec((tile, feat), lambda i: (i, 0)),
            pl.BlockSpec((feat, cols), lambda i: (0, 0)),
        ],
        out_shape=[
            jax.ShapeDtypeStruct((rows, feat), BF16),
            jax.ShapeDtypeStruct((rows, feat), BF16),
            jax.ShapeDtypeStruct((feat, cols), F32),
        ],
        compiler_params=params(dimension_semantics=("arbitrary",)),
        name="features",
    )(frames, weights, phases, residual)


def update_call(high, low, coef, residual, tile=256):
    rows, feat = high.shape
    cols = residual.shape[1]
    return pl.pallas_call(
        update_kernel,
        grid=(rows // tile,),
        in_specs=[
            pl.BlockSpec((tile, feat), lambda i: (i, 0)),
            pl.BlockSpec((tile, feat), lambda i: (i, 0)),
            pl.BlockSpec((feat, cols), lambda i: (0, 0)),
            pl.BlockSpec((tile, cols), lambda i: (i, 0)),
        ],
        out_specs=pl.BlockSpec((tile, cols), lambda i: (i, 0)),
        out_shape=jax.ShapeDtypeStruct((rows, cols), F32),
        compiler_params=params(dimension_semantics=("arbitrary",)),
        name="update",
    )(high, low, coef, residual)


def body(frames, weights, phases, residual):
    rows_here = frames.shape[0]
    feature_count = weights.shape[1]
    ridge = 0.1 * rows_here * lax.axis_size("rows") / feature_count
    phases = phases[None, :]
    gathered = lax.all_gather(frames, "tgt", axis=1, tiled=True)
    share = rows_here // lax.axis_size("tgt")
    own = lax.dynamic_slice_in_dim(gathered, lax.axis_index("tgt") * share, share, 0)
    pack = lax.psum(gram_call(own, weights, phases), ("rows", "tgt"))
    high, low, corr = feature_call(gathered, weights, phases, residual)
    corr = lax.psum(corr, "rows")
    panel, inverse = factor_call(pack, ridge)
    coefficients = solve_call(panel, inverse, corr)
    residual_next = update_call(high, low, coefficients, residual)
    return (residual_next, coefficients)


def solution(mesh):
    return jax.shard_map(
        body,
        mesh=mesh,
        in_specs=(P("rows", "tgt"), P(), P(), P("rows", "tgt")),
        out_specs=(P("rows", "tgt"), P(None, "tgt")),
        check_vma=False,
    )
```

```python
import math

import jax
import jax.numpy as jnp
from jax import lax
from jax.experimental import pallas as pl
from jax.experimental.pallas import tpu as pltpu
from jax.sharding import PartitionSpec as P

F32 = jnp.float32
BF16 = jnp.bfloat16
HIGHEST = lax.Precision.HIGHEST
NB = 128
PB = 16
SIN_PI = (
    3.1415926535362892,
    -5.167712764624528,
    2.5501633189472983,
    -0.5992521978285216,
    0.08205040183240117,
    -0.007028386446239114,
)


def dot(a, b, precision=None):
    return lax.dot_general(
        a, b, (((1,), (0,)), ((), ())), precision=precision, preferred_element_type=F32
    )


def dot_t(a, b, precision=None):
    return lax.dot_general(
        a, b, (((0,), (0,)), ((), ())), precision=precision, preferred_element_type=F32
    )


def split2(x):
    high = x.astype(BF16)
    return high, (x - high.astype(F32)).astype(BF16)


def split3(x):
    high = x.astype(BF16)
    rest = x - high.astype(F32)
    mid = rest.astype(BF16)
    return high, mid, (rest - mid.astype(F32)).astype(BF16)


def features(frames, weights, phases):
    turns = (dot(frames, weights) + phases) * (0.5 / math.pi)
    r = turns - jnp.round(turns)
    s = r * r
    poly = jnp.full_like(s, SIN_PI[-1])
    for coef in SIN_PI[-2::-1]:
        poly = poly * s + coef
    half = poly * r
    scale = math.sqrt(2.0 / weights.shape[1])
    return scale - (2.0 * scale) * (half * half)


def packed_slot(block, blocks):
    if block < blocks // 2:
        return block, 0
    return blocks - 1 - block, (block + 1) * NB


def gram_kernel(frames, weights, phases, out, high, low):
    blocks = out.shape[0] * 2
    slabs = jnp.concatenate([frames[i] for i in range(frames.shape[0])], axis=1)
    h, l = split2(features(slabs, weights[...], phases[...]))
    high[...] = h
    low[...] = l
    for i in range(blocks):
        rows = slice(i * NB, (i + 1) * NB)
        right = slice(i * NB, blocks * NB)
        g = dot_t(high[:, rows], high[:, right])
        g = g + dot_t(high[:, rows], low[:, right])
        g = g + dot_t(low[:, rows], high[:, right])
        at, col = packed_slot(i, blocks)
        out[at, :, col : col + (blocks - i) * NB] = g


def feature_kernel(order, own, left, right, far, weights, phases, residual, high, low, corr):
    slabs = jnp.concatenate([own[...], left[...], right[...], far[...]], axis=1)
    sorted_weights = jnp.concatenate([weights[order[i]] for i in range(4)], axis=0)
    h, l = split2(features(slabs, sorted_weights, phases[...]))
    high[...] = h
    low[...] = l
    rh, rl = split2(residual[...])
    part = dot_t(h, rh) + dot_t(h, rl) + dot_t(l, rh)

    @pl.when(pl.program_id(0) == 0)
    def _():
        corr[...] = part

    @pl.when(pl.program_id(0) > 0)
    def _():
        corr[...] += part


def invert_block(d):
    lane = lax.broadcasted_iota(jnp.int32, (PB, NB), 1)
    sub = lax.broadcasted_iota(jnp.int32, (PB, NB), 0)
    col_at = lax.broadcasted_iota(jnp.int32, (NB, NB), 1)
    zero = jnp.zeros((PB, NB), F32)
    for k0 in range(0, NB, PB):
        rows = d[k0 : k0 + PB, :]
        cols = [jnp.broadcast_to(rows[:, k0 + j : k0 + j + 1], (PB, NB)) for j in range(PB)]
        lh, lm, ll = split3(jnp.where(lane < k0, -rows, rows))
        left = jnp.concatenate([lh, lh, lm, lm, lh, ll], axis=0)
        x = jnp.where((lane >= k0) & (lane < k0 + PB), jnp.where(lane - k0 == sub, 1.0, 0.0), rows)
        scale = zero
        for k in range(PB):
            c = cols[k]
            p = 1.0 / c[k : k + 1, :]
            m = jnp.where(sub == k, 0.0, c * p)
            scale = jnp.where(sub == k, p, scale)
            for j in range(k + 1, PB):
                cols[j] = cols[j] - m * cols[j][k : k + 1, :]
            x = x - m * x[k : k + 1, :]
        x = x * scale
        xh, xm, xl = split3(x)
        right = jnp.concatenate([xh, xm, xh, xm, xl, xh], axis=0)
        update = dot_t(left, right)
        kept = d[...]
        d[...] = jnp.where((col_at >= k0) & (col_at < k0 + PB), 0.0, kept) - update
        d[k0 : k0 + PB, :] = x


def factor_kernel(core, mine, other, panel, inverse, a, d, *, ridge):
    blocks = panel.shape[0]
    size = blocks * NB
    quarter = blocks // 4

    def unpack(halves):
        for i in range(blocks):
            at, col = packed_slot(i, blocks)
            a[i, :, i * NB : size] = halves[at // quarter][at % quarter, :, col : col + size - i * NB]

    @pl.when(core[0] == 0)
    def _():
        unpack((mine, other))

    @pl.when(core[0] != 0)
    def _():
        unpack((other, mine))

    for i in range(blocks):
        if i > 0:
            a[i, :, : i * NB] = jnp.zeros((NB, i * NB), F32)
            panel[i, :, : i * NB] = jnp.zeros((NB, i * NB), F32)
    eye = jnp.where(
        lax.broadcasted_iota(jnp.int32, (NB, NB), 0) == lax.broadcasted_iota(jnp.int32, (NB, NB), 1),
        ridge,
        0.0,
    ).astype(F32)

    def step(i, _):
        own = pl.ds(pl.multiple_of(i * NB, NB), NB)
        d[...] = a[i, :, own] + eye
        invert_block(d)
        inverse[i] = d[...]

        def eliminate(first):
            panel[i, :, first:] = dot(d[...], a[i, :, first:], HIGHEST)

            def row(j, _):
                left = a[i, :, pl.ds(pl.multiple_of(j * NB, NB), NB)]
                a[j, :, first:] = a[j, :, first:] - dot_t(left, panel[i, :, first:], HIGHEST)
                return 0

            lax.fori_loop(i + 1, blocks, row, 0)

        for part in range(4):
            low = part * (blocks // 4)

            @pl.when((i >= low) & (i < low + blocks // 4))
            def _():
                eliminate(low * NB)

        return 0

    lax.fori_loop(0, blocks, step, 0)


def solve_kernel(panel, inverse, corr, out, c):
    blocks = panel.shape[0]
    c[...] = jnp.zeros_like(c)
    for i in range(blocks):
        rows = slice(i * NB, (i + 1) * NB)
        value = corr[rows, :]
        for j in range(i):
            value = value - dot_t(panel[j, :, rows], c[j * NB : (j + 1) * NB, :], HIGHEST)
        c[rows, :] = value
    for i in range(blocks - 1, -1, -1):
        rows = slice(i * NB, (i + 1) * NB)
        value = dot(inverse[i], c[rows, :], HIGHEST)
        if i < blocks - 1:
            rest = (i + 1) * NB
            value = value - dot(panel[i, :, rest:], out[rest:, :], HIGHEST)
        out[rows, :] = value


def update_kernel(high, low, coef, residual, out):
    wh, wl = split2(coef[...])
    h = high[...]
    out[...] = residual[...] - (dot(h, wh) + dot(h, wl) + dot(low[...], wh))


def params(**kw):
    return pltpu.CompilerParams(vmem_limit_bytes=56 * 1024 * 1024, **kw)


def factor_call(core, mine, other, ridge):
    blocks = mine.shape[0] * 4
    vmem = pl.BlockSpec(memory_space=pltpu.VMEM)
    return pl.pallas_call(
        lambda *refs: factor_kernel(*refs, ridge=ridge),
        in_specs=[pl.BlockSpec(memory_space=pltpu.SMEM), vmem, vmem],
        out_shape=(
            jax.ShapeDtypeStruct((blocks, NB, blocks * NB), F32),
            jax.ShapeDtypeStruct((blocks, NB, NB), F32),
        ),
        scratch_shapes=[
            pltpu.VMEM((blocks, NB, blocks * NB), F32),
            pltpu.VMEM((NB, NB), F32),
        ],
        compiler_params=params(),
        name="factor",
    )(core, mine, other)


def solve_call(panel, inverse, corr):
    return pl.pallas_call(
        solve_kernel,
        out_shape=jax.ShapeDtypeStruct(corr.shape, F32),
        scratch_shapes=[pltpu.VMEM(corr.shape, F32)],
        compiler_params=params(),
        name="solve",
    )(panel, inverse, corr)


def gram_call(frames, weights, phases):
    rows = frames.shape[1]
    feat = weights.shape[1]
    blocks = feat // NB
    return pl.pallas_call(
        gram_kernel,
        out_shape=jax.ShapeDtypeStruct((blocks // 2, NB, feat + NB), F32),
        scratch_shapes=[pltpu.VMEM((rows, feat), BF16), pltpu.VMEM((rows, feat), BF16)],
        compiler_params=params(),
        name="gram",
    )(frames, weights, phases)


def feature_call(order, slabs, weights, phases, residual, tile=256):
    rows, width = slabs[0].shape
    feat = weights.shape[1]
    cols = residual.shape[1]
    return pl.pallas_call(
        feature_kernel,
        grid=(rows // tile,),
        in_specs=[
            pl.BlockSpec(memory_space=pltpu.SMEM),
            *[pl.BlockSpec((tile, width), lambda i: (i, 0))] * 4,
            pl.BlockSpec((4, width, feat), lambda i: (0, 0, 0)),
            pl.BlockSpec((1, feat), lambda i: (0, 0)),
            pl.BlockSpec((tile, cols), lambda i: (i, 0)),
        ],
        out_specs=[
            pl.BlockSpec((tile, feat), lambda i: (i, 0)),
            pl.BlockSpec((tile, feat), lambda i: (i, 0)),
            pl.BlockSpec((feat, cols), lambda i: (0, 0)),
        ],
        out_shape=[
            jax.ShapeDtypeStruct((rows, feat), BF16),
            jax.ShapeDtypeStruct((rows, feat), BF16),
            jax.ShapeDtypeStruct((feat, cols), F32),
        ],
        compiler_params=params(dimension_semantics=("arbitrary",)),
        name="features",
    )(order, *slabs, weights.reshape(4, width, feat), phases, residual)


def update_call(high, low, coef, residual, tile=256):
    rows, feat = high.shape
    cols = residual.shape[1]
    return pl.pallas_call(
        update_kernel,
        grid=(rows // tile,),
        in_specs=[
            pl.BlockSpec((tile, feat), lambda i: (i, 0)),
            pl.BlockSpec((tile, feat), lambda i: (i, 0)),
            pl.BlockSpec((feat, cols), lambda i: (0, 0)),
            pl.BlockSpec((tile, cols), lambda i: (i, 0)),
        ],
        out_specs=pl.BlockSpec((tile, cols), lambda i: (i, 0)),
        out_shape=jax.ShapeDtypeStruct((rows, cols), F32),
        compiler_params=params(dimension_semantics=("arbitrary",)),
        name="update",
    )(high, low, coef, residual)


UP = [(i, (i + 1) % 4) for i in range(4)]
DOWN = [(i, (i - 1) % 4) for i in range(4)]
SWAP = [(0, 1), (1, 0)]


def exchange(parts, axes):
    return lax.all_to_all(parts, axes, 0, 0, tiled=True)


def to_everyone(value, axes):
    return exchange(jnp.broadcast_to(value[None], (lax.axis_size(axes), *value.shape)), axes)


def ring_slabs(own):
    left = lax.ppermute(own, "tgt", UP)
    right = lax.ppermute(own, "tgt", DOWN)
    half = own.shape[0] // 2
    far_top = lax.ppermute(left[:half], "tgt", UP)
    far_bottom = lax.ppermute(right[half:], "tgt", DOWN)
    return left, right, jnp.concatenate([far_top, far_bottom], axis=0)


def summed_gram(pack, core):
    halves = pack.reshape(2, -1, *pack.shape[1:])
    mine = lax.dynamic_index_in_dim(halves, core, 0, keepdims=False)
    other = lax.dynamic_index_in_dim(halves, 1 - core, 0, keepdims=False)
    mine = mine + lax.ppermute(other, "core", SWAP)
    chips = ("y", "z", "tgt")
    count = lax.axis_size(chips)
    parts = mine.reshape(count, -1, mine.shape[-1])
    piece = jnp.sum(exchange(parts, chips), axis=0)
    mine = to_everyone(piece, chips).reshape(mine.shape)
    return mine, lax.ppermute(mine, "core", SWAP)


def summed_corr(corr):
    plane = ("y", "z")
    count = lax.axis_size(plane)
    piece = jnp.sum(exchange(corr.reshape(count, -1, corr.shape[-1]), plane), axis=0)
    piece = piece + lax.ppermute(piece, "core", SWAP)
    return to_everyone(piece, plane).reshape(corr.shape)


def body(frames, weights, phases, residual):
    rows_here = frames.shape[0]
    feature_count = weights.shape[1]
    ridge = 0.1 * rows_here * lax.axis_size(("y", "z", "core")) / feature_count
    phases = phases[None, :]
    core = lax.axis_index("core")
    at = lax.axis_index("tgt")
    whole_rows = exchange(frames.reshape(4, rows_here // 4, -1), "tgt")
    whole_rows, own = lax.optimization_barrier((whole_rows, frames))
    slabs = (own, *ring_slabs(own))
    pack = gram_call(whole_rows, weights, phases)
    mine, other = summed_gram(pack, core)
    order = jnp.stack([at, at + 3, at + 1, at + 2]) % 4
    high, low, corr = feature_call(order, slabs, weights, phases, residual)
    corr = summed_corr(corr)
    panel, inverse = factor_call(core[None], mine, other, ridge)
    coefficients = solve_call(panel, inverse, corr)
    residual_next = update_call(high, low, coefficients, residual)
    return (residual_next, coefficients)


def solution(mesh):
    rows = ("y", "z", "core")
    mesh = jax.sharding.Mesh(mesh.devices.reshape(4, 4, 2, 4), (*rows, "tgt"))
    return jax.shard_map(
        body,
        mesh=mesh,
        in_specs=(P(rows, "tgt"), P(), P(), P(rows, "tgt")),
        out_specs=(P(rows, "tgt"), P(None, "tgt")),
        check_vma=False,
    )
```

```python
import math

import jax
import jax.numpy as jnp
from jax import lax
from jax.experimental import pallas as pl
from jax.experimental.pallas import tpu as pltpu
from jax.sharding import PartitionSpec as P


F32 = jnp.float32
BF16 = jnp.bfloat16
HIGHEST = lax.Precision.HIGHEST
NB = 128
PB = 16
SIN_PI = (
    3.1415926535362892,
    -5.167712764624528,
    2.5501633189472983,
    -0.5992521978285216,
    0.08205040183240117,
    -0.007028386446239114,
)


def dot(a, b, precision=None):
    return lax.dot_general(
        a, b, (((1,), (0,)), ((), ())), precision=precision, preferred_element_type=F32
    )


def dot_t(a, b, precision=None):
    return lax.dot_general(
        a, b, (((0,), (0,)), ((), ())), precision=precision, preferred_element_type=F32
    )


def split2(x):
    high = x.astype(BF16)
    return high, (x - high.astype(F32)).astype(BF16)


def split3(x):
    high = x.astype(BF16)
    rest = x - high.astype(F32)
    mid = rest.astype(BF16)
    return high, mid, (rest - mid.astype(F32)).astype(BF16)


def features(frames, weights, phases):
    turns = (dot(frames, weights) + phases) * (0.5 / math.pi)
    r = turns - jnp.round(turns)
    s = r * r
    poly = jnp.full_like(s, SIN_PI[-1])
    for coef in SIN_PI[-2::-1]:
        poly = poly * s + coef
    half = poly * r
    scale = math.sqrt(2.0 / weights.shape[1])
    return scale - (2.0 * scale) * (half * half)


def packed_slot(block, blocks):
    if block < blocks // 2:
        return block, 0
    return blocks - 1 - block, (block + 1) * NB


def gram_kernel(frames, weights, phases, out, high, low):
    blocks = out.shape[0] * 2
    slabs = jnp.concatenate([frames[i] for i in range(frames.shape[0])], axis=1)
    h, l = split2(features(slabs, weights[...], phases[...]))
    high[...] = h
    low[...] = l
    for i in range(blocks):
        rows = slice(i * NB, (i + 1) * NB)
        right = slice(i * NB, blocks * NB)
        g = dot_t(high[:, rows], high[:, right])
        g = g + dot_t(high[:, rows], low[:, right])
        g = g + dot_t(low[:, rows], high[:, right])
        at, col = packed_slot(i, blocks)
        out[at, :, col : col + (blocks - i) * NB] = g


def feature_kernel(order, own, left, right, far, weights, phases, residual, high, low, corr):
    slabs = jnp.concatenate([own[...], left[...], right[...], far[...]], axis=1)
    sorted_weights = jnp.concatenate([weights[order[i]] for i in range(4)], axis=0)
    h, l = split2(features(slabs, sorted_weights, phases[...]))
    high[...] = h
    low[...] = l
    rh, rl = split2(residual[...])
    part = dot_t(h, rh) + dot_t(h, rl) + dot_t(l, rh)

    @pl.when(pl.program_id(0) == 0)
    def _():
        corr[...] = part

    @pl.when(pl.program_id(0) > 0)
    def _():
        corr[...] += part


def invert_block(d):
    lane = lax.broadcasted_iota(jnp.int32, (PB, NB), 1)
    sub = lax.broadcasted_iota(jnp.int32, (PB, NB), 0)
    col_at = lax.broadcasted_iota(jnp.int32, (NB, NB), 1)
    zero = jnp.zeros((PB, NB), F32)
    for k0 in range(0, NB, PB):
        rows = d[k0 : k0 + PB, :]
        cols = [jnp.broadcast_to(rows[:, k0 + j : k0 + j + 1], (PB, NB)) for j in range(PB)]
        lh, lm, ll = split3(jnp.where(lane < k0, -rows, rows))
        left = jnp.concatenate([lh, lh, lm, lm, lh, ll], axis=0)
        x = jnp.where((lane >= k0) & (lane < k0 + PB), jnp.where(lane - k0 == sub, 1.0, 0.0), rows)
        scale = zero
        for k in range(PB):
            c = cols[k]
            p = 1.0 / c[k : k + 1, :]
            m = jnp.where(sub == k, 0.0, c * p)
            scale = jnp.where(sub == k, p, scale)
            for j in range(k + 1, PB):
                cols[j] = cols[j] - m * cols[j][k : k + 1, :]
            x = x - m * x[k : k + 1, :]
        x = x * scale
        xh, xm, xl = split3(x)
        right = jnp.concatenate([xh, xm, xh, xm, xl, xh], axis=0)
        update = dot_t(left, right)
        kept = d[...]
        d[...] = jnp.where((col_at >= k0) & (col_at < k0 + PB), 0.0, kept) - update
        d[k0 : k0 + PB, :] = x


def factor_steps(panel, inverse, a, d, ridge):
    steps = panel.shape[0]
    blocks = a.shape[0]
    for i in range(1, blocks):
        a[i, :, : i * NB] = jnp.zeros((NB, i * NB), F32)
    eye = jnp.where(
        lax.broadcasted_iota(jnp.int32, (NB, NB), 0) == lax.broadcasted_iota(jnp.int32, (NB, NB), 1),
        ridge,
        0.0,
    ).astype(F32)

    def step(i, _):
        own = pl.ds(pl.multiple_of(i * NB, NB), NB)
        d[...] = a[i, :, own] + eye
        invert_block(d)
        inverse[i] = d[...]

        def eliminate(first):
            panel[i, :, first:] = dot(d[...], a[i, :, first:], HIGHEST)
            if first > 0:
                panel[i, :, :first] = jnp.zeros((NB, first), F32)

            def row(j, _):
                left = a[i, :, pl.ds(pl.multiple_of(j * NB, NB), NB)]
                a[j, :, first:] = a[j, :, first:] - dot_t(left, panel[i, :, first:], HIGHEST)
                return 0

            lax.fori_loop(i + 1, blocks, row, 0)

        for low in range(0, steps, 2):

            @pl.when((i >= low) & (i < low + 2))
            def _():
                eliminate(low * NB)

        return 0

    lax.fori_loop(0, steps, step, 0)


def first_factor_kernel(core, mine, other, panel, inverse, rest, a, d, *, ridge):
    blocks = a.shape[0]
    size = blocks * NB
    quarter = blocks // 4

    def unpack(halves):
        for i in range(blocks):
            at, col = packed_slot(i, blocks)
            a[i, :, i * NB : size] = halves[at // quarter][at % quarter, :, col : col + size - i * NB]

    @pl.when(core[0] == 0)
    def _():
        unpack((mine, other))

    @pl.when(core[0] != 0)
    def _():
        unpack((other, mine))

    factor_steps(panel, inverse, a, d, ridge)
    steps = panel.shape[0]
    for i in range(steps, blocks):
        rest[i - steps] = a[i, :, steps * NB :]


def second_factor_kernel(matrix, panel, inverse, a, d, *, ridge):
    a[...] = matrix[...]
    factor_steps(panel, inverse, a, d, ridge)


def solve_kernel(panel0, inverse0, panel1, inverse1, corr, out, c):
    half = panel0.shape[0]
    blocks = half + panel1.shape[0]

    def panel(i, first, last):
        if i < half:
            return panel0[i, :, first * NB : last * NB]
        return panel1[i - half, :, (first - half) * NB : (last - half) * NB]

    for i in range(blocks):
        rows = slice(i * NB, (i + 1) * NB)
        value = corr[rows, :]
        for j in range(i):
            value = value - dot_t(panel(j, i, i + 1), c[j * NB : (j + 1) * NB, :], HIGHEST)
        c[rows, :] = value
    for i in range(blocks - 1, -1, -1):
        rows = slice(i * NB, (i + 1) * NB)
        inverse = inverse0[i] if i < half else inverse1[i - half]
        value = dot(inverse, c[rows, :], HIGHEST)
        if i < blocks - 1:
            value = value - dot(panel(i, i + 1, blocks), out[(i + 1) * NB :, :], HIGHEST)
        out[rows, :] = value


def update_kernel(high, low, coef, residual, out):
    wh, wl = split2(coef[...])
    h = high[...]
    out[...] = residual[...] - (dot(h, wh) + dot(h, wl) + dot(low[...], wh))


def cost(us):
    return pl.CostEstimate(flops=int(us * 5e8), bytes_accessed=0, transcendentals=0)


def params(**kw):
    return pltpu.CompilerParams(vmem_limit_bytes=56 * 1024 * 1024, **kw)


def factor_shapes(steps, blocks):
    return (
        jax.ShapeDtypeStruct((steps, NB, blocks * NB), F32),
        jax.ShapeDtypeStruct((steps, NB, NB), F32),
    )


def factor_scratch(blocks):
    return [pltpu.VMEM((blocks, NB, blocks * NB), F32), pltpu.VMEM((NB, NB), F32)]


def first_factor_call(core, mine, other, ridge):
    blocks = mine.shape[0] * 4
    steps = blocks // 2
    vmem = pl.BlockSpec(memory_space=pltpu.VMEM)
    return pl.pallas_call(
        lambda *refs: first_factor_kernel(*refs, ridge=ridge),
        in_specs=[pl.BlockSpec(memory_space=pltpu.SMEM), vmem, vmem],
        out_shape=(
            *factor_shapes(steps, blocks),
            jax.ShapeDtypeStruct((blocks - steps, NB, (blocks - steps) * NB), F32),
        ),
        scratch_shapes=factor_scratch(blocks),
        compiler_params=params(),
        cost_estimate=cost(28),
        name="factor0",
    )(core, mine, other)


def second_factor_call(matrix, ridge):
    blocks = matrix.shape[0]
    return pl.pallas_call(
        lambda *refs: second_factor_kernel(*refs, ridge=ridge),
        out_shape=factor_shapes(blocks, blocks),
        scratch_shapes=factor_scratch(blocks),
        compiler_params=params(),
        cost_estimate=cost(22),
        name="factor1",
    )(matrix)


def solve_call(factors, corr):
    return pl.pallas_call(
        solve_kernel,
        out_shape=jax.ShapeDtypeStruct(corr.shape, F32),
        scratch_shapes=[pltpu.VMEM(corr.shape, F32)],
        compiler_params=params(),
        cost_estimate=cost(12),
        name="solve",
    )(*factors, corr)


def gram_call(frames, weights, phases):
    rows = frames.shape[1]
    feat = weights.shape[1]
    blocks = feat // NB
    return pl.pallas_call(
        gram_kernel,
        out_shape=jax.ShapeDtypeStruct((blocks // 2, NB, feat + NB), F32),
        scratch_shapes=[pltpu.VMEM((rows, feat), BF16), pltpu.VMEM((rows, feat), BF16)],
        compiler_params=params(),
        cost_estimate=cost(7),
        name="gram",
    )(frames, weights, phases)


def feature_call(order, slabs, weights, phases, residual, tile=256):
    rows, width = slabs[0].shape
    feat = weights.shape[1]
    cols = residual.shape[1]
    return pl.pallas_call(
        feature_kernel,
        grid=(rows // tile,),
        in_specs=[
            pl.BlockSpec(memory_space=pltpu.SMEM),
            *[pl.BlockSpec((tile, width), lambda i: (i, 0))] * 4,
            pl.BlockSpec((4, width, feat), lambda i: (0, 0, 0)),
            pl.BlockSpec((1, feat), lambda i: (0, 0)),
            pl.BlockSpec((tile, cols), lambda i: (i, 0)),
        ],
        out_specs=[
            pl.BlockSpec((tile, feat), lambda i: (i, 0)),
            pl.BlockSpec((tile, feat), lambda i: (i, 0)),
            pl.BlockSpec((feat, cols), lambda i: (0, 0)),
        ],
        out_shape=[
            jax.ShapeDtypeStruct((rows, feat), BF16),
            jax.ShapeDtypeStruct((rows, feat), BF16),
            jax.ShapeDtypeStruct((feat, cols), F32),
        ],
        compiler_params=params(dimension_semantics=("arbitrary",)),
        cost_estimate=cost(15),
        name="features",
    )(order, *slabs, weights.reshape(4, width, feat), phases, residual)


def update_call(high, low, coef, residual, tile=256):
    rows, feat = high.shape
    cols = residual.shape[1]
    return pl.pallas_call(
        update_kernel,
        grid=(rows // tile,),
        in_specs=[
            pl.BlockSpec((tile, feat), lambda i: (i, 0)),
            pl.BlockSpec((tile, feat), lambda i: (i, 0)),
            pl.BlockSpec((feat, cols), lambda i: (0, 0)),
            pl.BlockSpec((tile, cols), lambda i: (i, 0)),
        ],
        out_specs=pl.BlockSpec((tile, cols), lambda i: (i, 0)),
        out_shape=jax.ShapeDtypeStruct((rows, cols), F32),
        compiler_params=params(dimension_semantics=("arbitrary",)),
        cost_estimate=cost(10),
        name="update",
    )(high, low, coef, residual)


UP = [(i, (i + 1) % 4) for i in range(4)]
DOWN = [(i, (i - 1) % 4) for i in range(4)]
SWAP = [(0, 1), (1, 0)]


def exchange(parts, axes):
    return lax.all_to_all(parts, axes, 0, 0, tiled=True)


def to_everyone(value, axes):
    return exchange(jnp.broadcast_to(value[None], (lax.axis_size(axes), *value.shape)), axes)


def ring_slabs(own):
    left = lax.ppermute(own, "tgt", UP)
    right = lax.ppermute(own, "tgt", DOWN)
    half = own.shape[0] // 2
    far_top = lax.ppermute(left[:half], "tgt", UP)
    far_bottom = lax.ppermute(right[half:], "tgt", DOWN)
    return left, right, jnp.concatenate([far_top, far_bottom], axis=0)


def summed_gram(pack, core):
    halves = pack.reshape(2, -1, *pack.shape[1:])
    mine = lax.dynamic_index_in_dim(halves, core, 0, keepdims=False)
    other = lax.dynamic_index_in_dim(halves, 1 - core, 0, keepdims=False)
    mine = mine + lax.ppermute(other, "core", SWAP)
    chips = ("y", "z", "tgt")
    count = lax.axis_size(chips)
    parts = mine.reshape(count, -1, mine.shape[-1])
    parts = exchange(parts, chips)
    piece = jnp.sum(parts, axis=0)
    mine = to_everyone(piece, chips).reshape(mine.shape)
    return mine, lax.ppermute(mine, "core", SWAP)


def summed_corr(corr):
    plane = ("y", "z")
    count = lax.axis_size(plane)
    parts = exchange(corr.reshape(count, -1, corr.shape[-1]), plane)
    piece = jnp.sum(parts, axis=0)
    piece = piece + lax.ppermute(piece, "core", SWAP)
    return to_everyone(piece, plane).reshape(corr.shape)


def block_step(frames, weights, phases, residual):
    rows_here = frames.shape[0]
    feature_count = weights.shape[1]
    ridge = 0.1 * rows_here * lax.axis_size(("y", "z", "core")) / feature_count
    phases = phases[None, :]
    core = lax.axis_index("core")
    at = lax.axis_index("tgt")
    whole_rows = exchange(frames.reshape(4, rows_here // 4, -1), "tgt")
    whole_rows, own = lax.optimization_barrier((whole_rows, frames))
    slabs = (own, *ring_slabs(own))
    pack = gram_call(whole_rows, weights, phases)
    mine, other = summed_gram(pack, core)
    order = jnp.stack([at, at + 3, at + 1, at + 2]) % 4
    high, low, corr = feature_call(order, slabs, weights, phases, residual)
    corr = summed_corr(corr)
    panel0, inverse0, rest = first_factor_call(core[None], mine, other, ridge)
    panel1, inverse1 = second_factor_call(rest, ridge)
    coefficients = solve_call((panel0, inverse0, panel1, inverse1), corr)
    residual_next = update_call(high, low, coefficients, residual)
    return (residual_next, coefficients)


def solution(mesh):
    rows = ("y", "z", "core")
    mesh = jax.sharding.Mesh(mesh.devices.reshape(4, 4, 2, 4), (*rows, "tgt"))
    return jax.shard_map(
        block_step,
        mesh=mesh,
        in_specs=(P(rows, "tgt"), P(), P(), P(rows, "tgt")),
        out_specs=(P(rows, "tgt"), P(None, "tgt")),
        check_vma=False,
    )
```

```python
import math

import jax
import jax.numpy as jnp
from jax import lax
from jax.experimental import pallas as pl
from jax.experimental.pallas import tpu as pltpu
from jax.sharding import PartitionSpec as P


F32 = jnp.float32
BF16 = jnp.bfloat16
HIGHEST = lax.Precision.HIGHEST
NB = 128
PB = 16
SIN_PI = (
    3.1415926535362892,
    -5.167712764624528,
    2.5501633189472983,
    -0.5992521978285216,
    0.08205040183240117,
    -0.007028386446239114,
)


def dot(a, b, precision=None):
    return lax.dot_general(
        a, b, (((1,), (0,)), ((), ())), precision=precision, preferred_element_type=F32
    )


def dot_t(a, b, precision=None):
    return lax.dot_general(
        a, b, (((0,), (0,)), ((), ())), precision=precision, preferred_element_type=F32
    )


def split2(x):
    high = x.astype(BF16)
    return high, (x - high.astype(F32)).astype(BF16)


def split3(x):
    high = x.astype(BF16)
    rest = x - high.astype(F32)
    mid = rest.astype(BF16)
    return high, mid, (rest - mid.astype(F32)).astype(BF16)


def dot3(a, b):
    return dot(a[0], b[0]) + (dot(a[0], b[1]) + dot(a[1], b[0]))


def dot3_t(a, b):
    return dot_t(a[0], b[0]) + (dot_t(a[0], b[1]) + dot_t(a[1], b[0]))


def features(frames, weights, phases):
    turns = (dot(frames, weights) + phases) * (0.5 / math.pi)
    r = turns - jnp.round(turns)
    s = r * r
    poly = jnp.full_like(s, SIN_PI[-1])
    for coef in SIN_PI[-2::-1]:
        poly = poly * s + coef
    half = poly * r
    scale = math.sqrt(2.0 / weights.shape[1])
    return scale - (2.0 * scale) * (half * half)


def packed_slot(block, blocks):
    if block < blocks // 2:
        return block, 0
    return blocks - 1 - block, (block + 1) * NB


def gram_kernel(frames, weights, phases, out, high, low):
    blocks = out.shape[0] * 2
    slabs = jnp.concatenate([frames[i] for i in range(frames.shape[0])], axis=1)
    h, l = split2(features(slabs, weights[...], phases[...]))
    high[...] = h
    low[...] = l
    for i in range(blocks):
        rows = slice(i * NB, (i + 1) * NB)
        right = slice(i * NB, blocks * NB)
        g = dot_t(high[:, rows], high[:, right])
        g = g + dot_t(high[:, rows], low[:, right])
        g = g + dot_t(low[:, rows], high[:, right])
        at, col = packed_slot(i, blocks)
        out[at, :, col : col + (blocks - i) * NB] = g


def feature_kernel(order, *refs):
    tops, bottoms, (weights, phases, residual, high, low, corr) = refs[:4], refs[4:8], refs[8:]
    below = pl.program_id(0) >= pl.num_programs(0) // 2
    slabs = [jnp.where(below, b[...], t[...]) for t, b in zip(tops, bottoms)]
    sorted_weights = jnp.concatenate([weights[order[i]] for i in range(4)], axis=0)
    h, l = split2(features(jnp.concatenate(slabs, axis=1), sorted_weights, phases[...]))
    high[...] = h
    low[...] = l
    right = split2(residual[...])
    part = dot3_t((h, l), right)

    @pl.when(pl.program_id(0) == 0)
    def _():
        corr[...] = part

    @pl.when(pl.program_id(0) > 0)
    def _():
        corr[...] += part


def invert_block(d):
    lane = lax.broadcasted_iota(jnp.int32, (PB, NB), 1)
    sub = lax.broadcasted_iota(jnp.int32, (PB, NB), 0)
    col_at = lax.broadcasted_iota(jnp.int32, (NB, NB), 1)
    zero = jnp.zeros((PB, NB), F32)
    for k0 in range(0, NB, PB):
        rows = d[k0 : k0 + PB, :]
        cols = [jnp.broadcast_to(rows[:, k0 + j : k0 + j + 1], (PB, NB)) for j in range(PB)]
        lh, lm, ll = split3(jnp.where(lane < k0, -rows, rows))
        left = jnp.concatenate([lh, lh, lm, lm, lh, ll], axis=0)
        x = jnp.where((lane >= k0) & (lane < k0 + PB), jnp.where(lane - k0 == sub, 1.0, 0.0), rows)
        scale = zero
        for k in range(PB):
            c = cols[k]
            p = 1.0 / c[k : k + 1, :]
            m = jnp.where(sub == k, 0.0, c * p)
            scale = jnp.where(sub == k, p, scale)
            for j in range(k + 1, PB):
                cols[j] = cols[j] - m * cols[j][k : k + 1, :]
            x = x - m * x[k : k + 1, :]
        x = x * scale
        xh, xm, xl = split3(x)
        right = jnp.concatenate([xh, xm, xh, xm, xl, xh], axis=0)
        update = dot_t(left, right)
        kept = d[...]
        d[...] = jnp.where((col_at >= k0) & (col_at < k0 + PB), 0.0, kept) - update
        d[k0 : k0 + PB, :] = x


def factor_steps(rows_of, panel, inverse, left, d, ridge):
    steps, _, width = panel[0].shape
    for ref in (*panel, *left):
        ref[...] = jnp.zeros_like(ref)
    eye = jnp.where(
        lax.broadcasted_iota(jnp.int32, (NB, NB), 0) == lax.broadcasted_iota(jnp.int32, (NB, NB), 1),
        ridge,
        0.0,
    ).astype(F32)

    def step(i, _):
        own = pl.ds(pl.multiple_of(i * NB, NB), NB)
        before = [ref[:, :, own].reshape(steps * NB, NB) for ref in left]
        done = [ref[...].reshape(steps * NB, width) for ref in panel]
        here = [ref[:, :, own].reshape(steps * NB, NB) for ref in panel]
        d[...] = rows_of(i, own) - dot3_t(before, here) + eye
        row = rows_of(i, slice(None)) - dot3_t(before, done)
        parts = split2(row)
        invert_block(d)
        inverse[i] = d[...]
        result = split2(dot(d[...], row, HIGHEST))
        for k in range(2):
            left[k][i] = parts[k]
            panel[k][i] = result[k]
        return 0

    lax.fori_loop(0, steps, step, 0)


def first_factor_kernel(core, mine, other, high, low, inverse, rest, a, lh, ll, d, *, ridge):
    blocks = a.shape[0]
    size = blocks * NB
    quarter = blocks // 4
    steps = high.shape[0]

    def unpack(halves):
        for i in range(blocks):
            at, col = packed_slot(i, blocks)
            a[i, :, i * NB : size] = halves[at // quarter][at % quarter, :, col : col + size - i * NB]

    @pl.when(core[0] == 0)
    def _():
        unpack((mine, other))

    @pl.when(core[0] != 0)
    def _():
        unpack((other, mine))

    for i in range(1, blocks):
        a[i, :, : i * NB] = jnp.zeros((NB, i * NB), F32)
    factor_steps(lambda i, cols: a[i, :, cols], (high, low), inverse, (lh, ll), d, ridge)
    edge = steps * NB
    right = [ref[:, :, edge:].reshape(edge, size - edge) for ref in (high, low)]
    for i in range(steps, blocks):
        cols = slice(i * NB, (i + 1) * NB)
        before = [ref[:, :, cols].reshape(edge, NB) for ref in (lh, ll)]
        rest[i - steps] = a[i, :, edge:] - dot3_t(before, right)


def second_factor_kernel(matrix, high, low, inverse, lh, ll, d, *, ridge):
    factor_steps(lambda i, cols: matrix[i, :, cols], (high, low), inverse, (lh, ll), d, ridge)


def solve_kernel(high0, low0, inverse0, high1, low1, inverse1, corr, out, ch, cl, wh, wl):
    half = high0.shape[0]
    blocks = half + high1.shape[0]
    edge = half * NB

    def store(parts, rows, value):
        for ref, part in zip(parts, split2(value)):
            ref[rows, :] = part

    def known(parts, first, last):
        return [ref[first * NB : last * NB, :] for ref in parts]

    for i in range(blocks):
        rows = slice(i * NB, (i + 1) * NB)
        value = corr[rows, :]
        top = min(i, half)
        if top > 0:
            left = [ref[:top, :, rows].reshape(top * NB, NB) for ref in (high0, low0)]
            value = value - dot3_t(left, known((ch, cl), 0, top))
        if i > half:
            cols = slice(i * NB - edge, (i + 1) * NB - edge)
            left = [ref[: i - half, :, cols].reshape((i - half) * NB, NB) for ref in (high1, low1)]
            value = value - dot3_t(left, known((ch, cl), half, i))
        store((ch, cl), rows, value)
    for i in range(blocks - 1, -1, -1):
        rows = slice(i * NB, (i + 1) * NB)
        inverse = inverse0[i] if i < half else inverse1[i - half]
        value = dot3(split2(inverse), known((ch, cl), i, i + 1))
        if i < blocks - 1:
            panel = (high0, low0) if i < half else (high1, low1)
            base = 0 if i < half else half
            right = [ref[i - base, :, (i + 1 - base) * NB :] for ref in panel]
            value = value - dot3(right, known((wh, wl), i + 1, blocks))
        out[rows, :] = value
        store((wh, wl), rows, value)


def update_kernel(high, low, coef, residual, out):
    wh, wl = split2(coef[...])
    h = high[...]
    out[...] = residual[...] - (dot(h, wh) + dot(h, wl) + dot(low[...], wh))


def cost(us):
    return pl.CostEstimate(flops=int(us * 5e8), bytes_accessed=0, transcendentals=0)


def params(**kw):
    return pltpu.CompilerParams(vmem_limit_bytes=28 * 1024 * 1024, **kw)


def factor_shapes(steps, blocks):
    return (
        jax.ShapeDtypeStruct((steps, NB, blocks * NB), BF16),
        jax.ShapeDtypeStruct((steps, NB, blocks * NB), BF16),
        jax.ShapeDtypeStruct((steps, NB, NB), F32),
    )


def factor_scratch(steps, blocks):
    return [
        pltpu.VMEM((steps, NB, blocks * NB), BF16),
        pltpu.VMEM((steps, NB, blocks * NB), BF16),
        pltpu.VMEM((NB, NB), F32),
    ]


def first_factor_call(core, mine, other, ridge):
    blocks = mine.shape[0] * 4
    steps = blocks // 2
    vmem = pl.BlockSpec(memory_space=pltpu.VMEM)
    return pl.pallas_call(
        lambda *refs: first_factor_kernel(*refs, ridge=ridge),
        in_specs=[pl.BlockSpec(memory_space=pltpu.SMEM), vmem, vmem],
        out_shape=(
            *factor_shapes(steps, blocks),
            jax.ShapeDtypeStruct((blocks - steps, NB, (blocks - steps) * NB), F32),
        ),
        scratch_shapes=[
            pltpu.VMEM((blocks, NB, blocks * NB), F32),
            *factor_scratch(steps, blocks),
        ],
        compiler_params=params(),
        cost_estimate=cost(28),
        name="factor0",
    )(core, mine, other)


def second_factor_call(matrix, ridge):
    blocks = matrix.shape[0]
    return pl.pallas_call(
        lambda *refs: second_factor_kernel(*refs, ridge=ridge),
        out_shape=factor_shapes(blocks, blocks),
        scratch_shapes=factor_scratch(blocks, blocks),
        compiler_params=params(),
        cost_estimate=cost(22),
        name="factor1",
    )(matrix)


def solve_call(factors, corr):
    return pl.pallas_call(
        solve_kernel,
        out_shape=jax.ShapeDtypeStruct(corr.shape, F32),
        scratch_shapes=[pltpu.VMEM(corr.shape, BF16) for _ in range(4)],
        compiler_params=params(),
        cost_estimate=cost(12),
        name="solve",
    )(*factors, corr)


def gram_call(frames, weights, phases):
    rows = frames.shape[1]
    feat = weights.shape[1]
    blocks = feat // NB
    return pl.pallas_call(
        gram_kernel,
        out_shape=jax.ShapeDtypeStruct((blocks // 2, NB, feat + NB), F32),
        scratch_shapes=[pltpu.VMEM((rows, feat), BF16), pltpu.VMEM((rows, feat), BF16)],
        compiler_params=params(),
        cost_estimate=cost(7),
        name="gram",
    )(frames, weights, phases)


def feature_call(order, tops, bottoms, weights, phases, residual, tile=256):
    rows, cols = residual.shape
    width = tops[0].shape[1]
    feat = weights.shape[1]
    half = rows // tile // 2
    return pl.pallas_call(
        feature_kernel,
        grid=(rows // tile,),
        in_specs=[
            pl.BlockSpec(memory_space=pltpu.SMEM),
            *[pl.BlockSpec((tile, width), lambda i: (jnp.minimum(i, half - 1), 0))] * 4,
            *[pl.BlockSpec((tile, width), lambda i: (jnp.maximum(i - half, 0), 0))] * 4,
            pl.BlockSpec((4, width, feat), lambda i: (0, 0, 0)),
            pl.BlockSpec((1, feat), lambda i: (0, 0)),
            pl.BlockSpec((tile, cols), lambda i: (i, 0)),
        ],
        out_specs=[
            pl.BlockSpec((tile, feat), lambda i: (i, 0)),
            pl.BlockSpec((tile, feat), lambda i: (i, 0)),
            pl.BlockSpec((feat, cols), lambda i: (0, 0)),
        ],
        out_shape=[
            jax.ShapeDtypeStruct((rows, feat), BF16),
            jax.ShapeDtypeStruct((rows, feat), BF16),
            jax.ShapeDtypeStruct((feat, cols), F32),
        ],
        compiler_params=params(dimension_semantics=("arbitrary",)),
        cost_estimate=cost(15),
        name="features",
    )(order, *tops, *bottoms, weights.reshape(4, width, feat), phases, residual)


def update_call(high, low, coef, residual, tile=256):
    rows, feat = high.shape
    cols = residual.shape[1]
    return pl.pallas_call(
        update_kernel,
        grid=(rows // tile,),
        in_specs=[
            pl.BlockSpec((tile, feat), lambda i: (i, 0)),
            pl.BlockSpec((tile, feat), lambda i: (i, 0)),
            pl.BlockSpec((feat, cols), lambda i: (0, 0)),
            pl.BlockSpec((tile, cols), lambda i: (i, 0)),
        ],
        out_specs=pl.BlockSpec((tile, cols), lambda i: (i, 0)),
        out_shape=jax.ShapeDtypeStruct((rows, cols), F32),
        compiler_params=params(dimension_semantics=("arbitrary",)),
        cost_estimate=cost(10),
        name="update",
    )(high, low, coef, residual)


UP = [(i, (i + 1) % 4) for i in range(4)]
DOWN = [(i, (i - 1) % 4) for i in range(4)]
SWAP = [(0, 1), (1, 0)]


def exchange(parts, axes):
    return lax.all_to_all(parts, axes, 0, 0, tiled=True)


def to_everyone(value, axes):
    return exchange(jnp.broadcast_to(value[None], (lax.axis_size(axes), *value.shape)), axes)


def ring_slabs(own):
    half = own.shape[0] // 2
    top, bottom = own[:half], own[half:]
    left_top = lax.ppermute(top, "tgt", UP)
    right_bottom = lax.ppermute(bottom, "tgt", DOWN)
    left_bottom = lax.ppermute(bottom, "tgt", UP)
    right_top = lax.ppermute(top, "tgt", DOWN)
    far_top = lax.ppermute(left_top, "tgt", UP)
    far_bottom = lax.ppermute(right_bottom, "tgt", DOWN)
    return (top, left_top, right_top, far_top), (bottom, left_bottom, right_bottom, far_bottom)


def summed_gram(pack, core):
    halves = pack.reshape(2, -1, *pack.shape[1:])
    mine = lax.dynamic_index_in_dim(halves, core, 0, keepdims=False)
    other = lax.dynamic_index_in_dim(halves, 1 - core, 0, keepdims=False)
    mine = mine + lax.ppermute(other, "core", SWAP)
    chips = ("y", "z", "tgt")
    count = lax.axis_size(chips)
    parts = mine.reshape(count, -1, mine.shape[-1])
    parts = exchange(parts, chips)
    piece = jnp.sum(parts, axis=0)
    mine = to_everyone(piece, chips).reshape(mine.shape)
    return mine, lax.ppermute(mine, "core", SWAP)


def summed_corr(corr):
    plane = ("y", "z")
    count = lax.axis_size(plane)
    parts = exchange(corr.reshape(count, -1, corr.shape[-1]), plane)
    piece = jnp.sum(parts, axis=0)
    piece = piece + lax.ppermute(piece, "core", SWAP)
    return to_everyone(piece, plane).reshape(corr.shape)


def block_step(frames, weights, phases, residual):
    rows_here = frames.shape[0]
    feature_count = weights.shape[1]
    ridge = 0.1 * rows_here * lax.axis_size(("y", "z", "core")) / feature_count
    phases = phases[None, :]
    core = lax.axis_index("core")
    at = lax.axis_index("tgt")
    whole_rows = exchange(frames.reshape(4, rows_here // 4, -1), "tgt")
    whole_rows, own = lax.optimization_barrier((whole_rows, frames))
    tops, bottoms = ring_slabs(own)
    pack = gram_call(whole_rows, weights, phases)
    mine, other = summed_gram(pack, core)
    order = jnp.stack([at, at + 3, at + 1, at + 2]) % 4
    high, low, corr = feature_call(order, tops, bottoms, weights, phases, residual)
    corr = summed_corr(corr)
    *factor0, rest = first_factor_call(core[None], mine, other, ridge)
    factor1 = second_factor_call(rest, ridge)
    coefficients = solve_call((*factor0, *factor1), corr)
    residual_next = update_call(high, low, coefficients, residual)
    return (residual_next, coefficients)


def solution(mesh):
    rows = ("y", "z", "core")
    mesh = jax.sharding.Mesh(mesh.devices.reshape(4, 4, 2, 4), (*rows, "tgt"))
    return jax.shard_map(
        block_step,
        mesh=mesh,
        in_specs=(P(rows, "tgt"), P(), P(), P(rows, "tgt")),
        out_specs=(P(rows, "tgt"), P(None, "tgt")),
        check_vma=False,
    )
```

```python
import math

import jax
import jax.numpy as jnp
from jax import lax
from jax.experimental import pallas as pl
from jax.experimental.pallas import tpu as pltpu
from jax.sharding import PartitionSpec as P


F32 = jnp.float32
BF16 = jnp.bfloat16
HIGHEST = lax.Precision.HIGHEST
NB = 128
PB = 16
SIN_PI = (
    3.1415926535362892,
    -5.167712764624528,
    2.5501633189472983,
    -0.5992521978285216,
    0.08205040183240117,
    -0.007028386446239114,
)


def dot(a, b, precision=None):
    return lax.dot_general(
        a, b, (((1,), (0,)), ((), ())), precision=precision, preferred_element_type=F32
    )


def dot_t(a, b, precision=None):
    return lax.dot_general(
        a, b, (((0,), (0,)), ((), ())), precision=precision, preferred_element_type=F32
    )


def split2(x):
    high = x.astype(BF16)
    return high, (x - high.astype(F32)).astype(BF16)


def split3(x):
    high = x.astype(BF16)
    rest = x - high.astype(F32)
    mid = rest.astype(BF16)
    return high, mid, (rest - mid.astype(F32)).astype(BF16)


def dot3(a, b):
    return dot(a[0], b[0]) + (dot(a[0], b[1]) + dot(a[1], b[0]))


def dot3_t(a, b):
    return dot_t(a[0], b[0]) + (dot_t(a[0], b[1]) + dot_t(a[1], b[0]))


def features(frames, weights, phases):
    turns = (dot(frames, weights) + phases) * (0.5 / math.pi)
    r = turns - jnp.round(turns)
    s = r * r
    poly = jnp.full_like(s, SIN_PI[-1])
    for coef in SIN_PI[-2::-1]:
        poly = poly * s + coef
    half = poly * r
    scale = math.sqrt(2.0 / weights.shape[1])
    return scale - (2.0 * scale) * (half * half)


def packed_slot(block, blocks):
    if block < blocks // 2:
        return block, 0
    return blocks - 1 - block, (block + 1) * NB


def gram_kernel(core, frames, weights, phases, mine, other, high, low):
    quarter = mine.shape[0]
    blocks = quarter * 4
    slabs = jnp.concatenate([frames[i] for i in range(frames.shape[0])], axis=1)
    h, l = split2(features(slabs, weights[...], phases[...]))
    high[...] = h
    low[...] = l
    for i in range(blocks):
        rows = slice(i * NB, (i + 1) * NB)
        right = slice(i * NB, blocks * NB)
        g = dot_t(high[:, rows], high[:, right])
        g = g + dot_t(high[:, rows], low[:, right])
        g = g + dot_t(low[:, rows], high[:, right])
        at, col = packed_slot(i, blocks)
        own = core[0] == at // quarter

        def store(half):
            half[at % quarter, :, col : col + (blocks - i) * NB] = g

        pl.when(own)(lambda: store(mine))
        pl.when(jnp.logical_not(own))(lambda: store(other))


def feature_kernel(order, *refs):
    tops, bottoms, (weights, phases, residual, high, low, corr) = refs[:4], refs[4:8], refs[8:]
    below = pl.program_id(0) >= pl.num_programs(0) // 2
    slabs = [jnp.where(below, b[...], t[...]) for t, b in zip(tops, bottoms)]
    sorted_weights = jnp.concatenate([weights[order[i]] for i in range(4)], axis=0)
    h, l = split2(features(jnp.concatenate(slabs, axis=1), sorted_weights, phases[...]))
    high[...] = h
    low[...] = l
    right = split2(residual[...])
    part = dot3_t((h, l), right)

    @pl.when(pl.program_id(0) == 0)
    def _():
        corr[...] = part

    @pl.when(pl.program_id(0) > 0)
    def _():
        corr[...] += part


def invert_block(d):
    lane = lax.broadcasted_iota(jnp.int32, (PB, NB), 1)
    sub = lax.broadcasted_iota(jnp.int32, (PB, NB), 0)
    col_at = lax.broadcasted_iota(jnp.int32, (NB, NB), 1)
    zero = jnp.zeros((PB, NB), F32)
    for k0 in range(0, NB, PB):
        rows = d[k0 : k0 + PB, :]
        cols = [jnp.broadcast_to(rows[:, k0 + j : k0 + j + 1], (PB, NB)) for j in range(PB)]
        lh, lm, ll = split3(jnp.where(lane < k0, -rows, rows))
        left = jnp.concatenate([lh, lh, lm, lm, lh, ll], axis=0)
        x = jnp.where((lane >= k0) & (lane < k0 + PB), jnp.where(lane - k0 == sub, 1.0, 0.0), rows)
        scale = zero
        for k in range(PB):
            c = cols[k]
            p = 1.0 / c[k : k + 1, :]
            m = jnp.where(sub == k, 0.0, c * p)
            scale = jnp.where(sub == k, p, scale)
            for j in range(k + 1, PB):
                cols[j] = cols[j] - m * cols[j][k : k + 1, :]
            x = x - m * x[k : k + 1, :]
        x = x * scale
        xh, xm, xl = split3(x)
        right = jnp.concatenate([xh, xm, xh, xm, xl, xh], axis=0)
        update = dot_t(left, right)
        kept = d[...]
        d[...] = jnp.where((col_at >= k0) & (col_at < k0 + PB), 0.0, kept) - update
        d[k0 : k0 + PB, :] = x


def factor_steps(rows_of, panel, inverse, left, d, ridge):
    steps, _, width = panel[0].shape
    for ref in (*panel, *left):
        ref[...] = jnp.zeros_like(ref)
    eye = jnp.where(
        lax.broadcasted_iota(jnp.int32, (NB, NB), 0) == lax.broadcasted_iota(jnp.int32, (NB, NB), 1),
        ridge,
        0.0,
    ).astype(F32)

    def step(i, _):
        own = pl.ds(pl.multiple_of(i * NB, NB), NB)
        before = [ref[:, :, own].reshape(steps * NB, NB) for ref in left]
        done = [ref[...].reshape(steps * NB, width) for ref in panel]
        here = [ref[:, :, own].reshape(steps * NB, NB) for ref in panel]
        d[...] = rows_of(i, own) - dot3_t(before, here) + eye
        row = rows_of(i, slice(None)) - dot3_t(before, done)
        parts = split2(row)
        invert_block(d)
        inverse[i] = d[...]
        result = split2(dot(d[...], row, HIGHEST))
        for k in range(2):
            left[k][i] = parts[k]
            panel[k][i] = result[k]
        return 0

    lax.fori_loop(0, steps, step, 0)


def first_factor_kernel(core, mine, other, high, low, inverse, rest, a, lh, ll, d, *, ridge):
    blocks = a.shape[0]
    size = blocks * NB
    quarter = blocks // 4
    steps = high.shape[0]

    def unpack(halves):
        for i in range(blocks):
            at, col = packed_slot(i, blocks)
            a[i, :, i * NB : size] = halves[at // quarter][at % quarter, :, col : col + size - i * NB]

    @pl.when(core[0] == 0)
    def _():
        unpack((mine, other))

    @pl.when(core[0] != 0)
    def _():
        unpack((other, mine))

    for i in range(1, blocks):
        a[i, :, : i * NB] = jnp.zeros((NB, i * NB), F32)
    factor_steps(lambda i, cols: a[i, :, cols], (high, low), inverse, (lh, ll), d, ridge)
    edge = steps * NB
    right = [ref[:, :, edge:].reshape(edge, size - edge) for ref in (high, low)]
    for i in range(steps, blocks):
        cols = slice(i * NB, (i + 1) * NB)
        before = [ref[:, :, cols].reshape(edge, NB) for ref in (lh, ll)]
        rest[i - steps] = a[i, :, edge:] - dot3_t(before, right)


def second_factor_kernel(matrix, high, low, inverse, lh, ll, d, *, ridge):
    factor_steps(lambda i, cols: matrix[i, :, cols], (high, low), inverse, (lh, ll), d, ridge)


def solve_kernel(high0, low0, inverse0, high1, low1, inverse1, corr, out, ch, cl, wh, wl):
    half = high0.shape[0]
    blocks = half + high1.shape[0]
    edge = half * NB

    def store(parts, rows, value):
        for ref, part in zip(parts, split2(value)):
            ref[rows, :] = part

    def known(parts, first, last):
        return [ref[first * NB : last * NB, :] for ref in parts]

    for i in range(blocks):
        rows = slice(i * NB, (i + 1) * NB)
        value = corr[rows, :]
        top = min(i, half)
        if top > 0:
            left = [ref[:top, :, rows].reshape(top * NB, NB) for ref in (high0, low0)]
            value = value - dot3_t(left, known((ch, cl), 0, top))
        if i > half:
            cols = slice(i * NB - edge, (i + 1) * NB - edge)
            left = [ref[: i - half, :, cols].reshape((i - half) * NB, NB) for ref in (high1, low1)]
            value = value - dot3_t(left, known((ch, cl), half, i))
        store((ch, cl), rows, value)
    for i in range(blocks - 1, -1, -1):
        rows = slice(i * NB, (i + 1) * NB)
        inverse = inverse0[i] if i < half else inverse1[i - half]
        value = dot3(split2(inverse), known((ch, cl), i, i + 1))
        if i < blocks - 1:
            panel = (high0, low0) if i < half else (high1, low1)
            base = 0 if i < half else half
            right = [ref[i - base, :, (i + 1 - base) * NB :] for ref in panel]
            value = value - dot3(right, known((wh, wl), i + 1, blocks))
        out[rows, :] = value
        store((wh, wl), rows, value)


def update_kernel(high, low, coef, residual, out):
    wh, wl = split2(coef[...])
    h = high[...]
    out[...] = residual[...] - (dot(h, wh) + dot(h, wl) + dot(low[...], wh))


def cost(us):
    return pl.CostEstimate(flops=int(us * 5e8), bytes_accessed=0, transcendentals=0)


def params(mib, **kw):
    return pltpu.CompilerParams(vmem_limit_bytes=mib * 1024 * 1024, **kw)


def factor_shapes(steps, blocks):
    return (
        jax.ShapeDtypeStruct((steps, NB, blocks * NB), BF16),
        jax.ShapeDtypeStruct((steps, NB, blocks * NB), BF16),
        jax.ShapeDtypeStruct((steps, NB, NB), F32),
    )


def factor_scratch(steps, blocks):
    return [
        pltpu.VMEM((steps, NB, blocks * NB), BF16),
        pltpu.VMEM((steps, NB, blocks * NB), BF16),
        pltpu.VMEM((NB, NB), F32),
    ]


def first_factor_call(core, mine, other, ridge):
    blocks = mine.shape[0] * 4
    steps = blocks // 2
    vmem = pl.BlockSpec(memory_space=pltpu.VMEM)
    return pl.pallas_call(
        lambda *refs: first_factor_kernel(*refs, ridge=ridge),
        in_specs=[pl.BlockSpec(memory_space=pltpu.SMEM), vmem, vmem],
        out_shape=(
            *factor_shapes(steps, blocks),
            jax.ShapeDtypeStruct((blocks - steps, NB, (blocks - steps) * NB), F32),
        ),
        scratch_shapes=[
            pltpu.VMEM((blocks, NB, blocks * NB), F32),
            *factor_scratch(steps, blocks),
        ],
        compiler_params=params(56),
        cost_estimate=cost(28),
        name="factor0",
    )(core, mine, other)


def second_factor_call(matrix, ridge):
    blocks = matrix.shape[0]
    return pl.pallas_call(
        lambda *refs: second_factor_kernel(*refs, ridge=ridge),
        out_shape=factor_shapes(blocks, blocks),
        scratch_shapes=factor_scratch(blocks, blocks),
        compiler_params=params(56),
        cost_estimate=cost(22),
        name="factor1",
    )(matrix)


def solve_call(factors, corr):
    return pl.pallas_call(
        solve_kernel,
        out_shape=jax.ShapeDtypeStruct(corr.shape, F32),
        scratch_shapes=[pltpu.VMEM(corr.shape, BF16) for _ in range(4)],
        compiler_params=params(28),
        cost_estimate=cost(12),
        name="solve",
    )(*factors, corr)


def gram_call(core, frames, weights, phases):
    rows = frames.shape[1]
    feat = weights.shape[1]
    vmem = pl.BlockSpec(memory_space=pltpu.VMEM)
    half = jax.ShapeDtypeStruct((feat // NB // 4, NB, feat + NB), F32)
    return pl.pallas_call(
        gram_kernel,
        in_specs=[pl.BlockSpec(memory_space=pltpu.SMEM), vmem, vmem, vmem],
        out_shape=(half, half),
        scratch_shapes=[pltpu.VMEM((rows, feat), BF16), pltpu.VMEM((rows, feat), BF16)],
        compiler_params=params(28),
        cost_estimate=cost(7),
        name="gram",
    )(core, frames, weights, phases)


def feature_call(order, tops, bottoms, weights, phases, residual, tile=256):
    rows, cols = residual.shape
    width = tops[0].shape[1]
    feat = weights.shape[1]
    half = rows // tile // 2
    return pl.pallas_call(
        feature_kernel,
        grid=(rows // tile,),
        in_specs=[
            pl.BlockSpec(memory_space=pltpu.SMEM),
            *[pl.BlockSpec((tile, width), lambda i: (jnp.minimum(i, half - 1), 0))] * 4,
            *[pl.BlockSpec((tile, width), lambda i: (jnp.maximum(i - half, 0), 0))] * 4,
            pl.BlockSpec((4, width, feat), lambda i: (0, 0, 0)),
            pl.BlockSpec((1, feat), lambda i: (0, 0)),
            pl.BlockSpec((tile, cols), lambda i: (i, 0)),
        ],
        out_specs=[
            pl.BlockSpec((tile, feat), lambda i: (i, 0)),
            pl.BlockSpec((tile, feat), lambda i: (i, 0)),
            pl.BlockSpec((feat, cols), lambda i: (0, 0)),
        ],
        out_shape=[
            jax.ShapeDtypeStruct((rows, feat), BF16),
            jax.ShapeDtypeStruct((rows, feat), BF16),
            jax.ShapeDtypeStruct((feat, cols), F32),
        ],
        compiler_params=params(56, dimension_semantics=("arbitrary",)),
        cost_estimate=cost(15),
        name="features",
    )(order, *tops, *bottoms, weights.reshape(4, width, feat), phases, residual)


def update_call(high, low, coef, residual, tile=256):
    rows, feat = high.shape
    cols = residual.shape[1]
    return pl.pallas_call(
        update_kernel,
        grid=(rows // tile,),
        in_specs=[
            pl.BlockSpec((tile, feat), lambda i: (i, 0)),
            pl.BlockSpec((tile, feat), lambda i: (i, 0)),
            pl.BlockSpec((feat, cols), lambda i: (0, 0)),
            pl.BlockSpec((tile, cols), lambda i: (i, 0)),
        ],
        out_specs=pl.BlockSpec((tile, cols), lambda i: (i, 0)),
        out_shape=jax.ShapeDtypeStruct((rows, cols), F32),
        compiler_params=params(28, dimension_semantics=("arbitrary",)),
        cost_estimate=cost(10),
        name="update",
    )(high, low, coef, residual)


UP = [(i, (i + 1) % 4) for i in range(4)]
DOWN = [(i, (i - 1) % 4) for i in range(4)]
SWAP = [(0, 1), (1, 0)]


def exchange(parts, axes):
    return lax.all_to_all(parts, axes, 0, 0, tiled=True)


def to_everyone(value, axes):
    return exchange(jnp.broadcast_to(value[None], (lax.axis_size(axes), *value.shape)), axes)


def ring_slabs(own):
    half = own.shape[0] // 2
    top, bottom = own[:half], own[half:]
    left_top = lax.ppermute(top, "tgt", UP)
    right_bottom = lax.ppermute(bottom, "tgt", DOWN)
    left_bottom = lax.ppermute(bottom, "tgt", UP)
    right_top = lax.ppermute(top, "tgt", DOWN)
    far_top = lax.ppermute(left_top, "tgt", UP)
    far_bottom = lax.ppermute(right_bottom, "tgt", DOWN)
    return (top, left_top, right_top, far_top), (bottom, left_bottom, right_bottom, far_bottom)


def summed_gram(mine, other):
    mine = mine + lax.ppermute(other, "core", SWAP)
    chips = ("y", "z", "tgt")
    count = lax.axis_size(chips)
    parts = mine.reshape(count, -1, mine.shape[-1])
    parts = exchange(parts, chips)
    piece = jnp.sum(parts, axis=0)
    mine = to_everyone(piece, chips).reshape(mine.shape)
    return mine, lax.ppermute(mine, "core", SWAP)


def summed_corr(corr):
    plane = ("y", "z")
    count = lax.axis_size(plane)
    parts = exchange(corr.reshape(count, -1, corr.shape[-1]), plane)
    piece = jnp.sum(parts, axis=0)
    piece = piece + lax.ppermute(piece, "core", SWAP)
    return to_everyone(piece, plane).reshape(corr.shape)


def block_step(frames, weights, phases, residual):
    rows_here = frames.shape[0]
    feature_count = weights.shape[1]
    ridge = 0.1 * rows_here * lax.axis_size(("y", "z", "core")) / feature_count
    phases = phases[None, :]
    core = lax.axis_index("core")
    at = lax.axis_index("tgt")
    whole_rows = exchange(frames.reshape(4, rows_here // 4, -1), "tgt")
    whole_rows, own = lax.optimization_barrier((whole_rows, frames))
    tops, bottoms = ring_slabs(own)
    halves = gram_call(core[None], whole_rows, weights, phases)
    mine, other = summed_gram(*halves)
    order = jnp.stack([at, at + 3, at + 1, at + 2]) % 4
    high, low, corr = feature_call(order, tops, bottoms, weights, phases, residual)
    corr = summed_corr(corr)
    *factor0, rest = first_factor_call(core[None], mine, other, ridge)
    factor1 = second_factor_call(rest, ridge)
    coefficients = solve_call((*factor0, *factor1), corr)
    residual_next = update_call(high, low, coefficients, residual)
    return (residual_next, coefficients)


def solution(mesh):
    rows = ("y", "z", "core")
    mesh = jax.sharding.Mesh(mesh.devices.reshape(4, 4, 2, 4), (*rows, "tgt"))
    return jax.shard_map(
        block_step,
        mesh=mesh,
        in_specs=(P(rows, "tgt"), P(), P(), P(rows, "tgt")),
        out_specs=(P(rows, "tgt"), P(None, "tgt")),
        check_vma=False,
    )
```

```python
import math

import jax
import jax.numpy as jnp
from jax import lax
from jax.experimental import pallas as pl
from jax.experimental.pallas import tpu as pltpu
from jax.sharding import PartitionSpec as P


F32 = jnp.float32
BF16 = jnp.bfloat16
HIGHEST = lax.Precision.HIGHEST
NB = 128
PB = 16
SIN_PI = (
    3.1415926535362892,
    -5.167712764624528,
    2.5501633189472983,
    -0.5992521978285216,
    0.08205040183240117,
    -0.007028386446239114,
)


def dot(a, b, precision=None):
    return lax.dot_general(
        a, b, (((1,), (0,)), ((), ())), precision=precision, preferred_element_type=F32
    )


def dot_t(a, b, precision=None):
    return lax.dot_general(
        a, b, (((0,), (0,)), ((), ())), precision=precision, preferred_element_type=F32
    )


def split2(x):
    high = x.astype(BF16)
    return high, (x - high.astype(F32)).astype(BF16)


def split3(x):
    high = x.astype(BF16)
    rest = x - high.astype(F32)
    mid = rest.astype(BF16)
    return high, mid, (rest - mid.astype(F32)).astype(BF16)


def dot3(a, b):
    return dot(a[0], b[0]) + (dot(a[0], b[1]) + dot(a[1], b[0]))


def dot3_t(a, b):
    return dot_t(a[0], b[0]) + (dot_t(a[0], b[1]) + dot_t(a[1], b[0]))


def features(frames, weights, phases):
    turns = (dot(frames, weights) + phases) * (0.5 / math.pi)
    r = turns - jnp.round(turns)
    s = r * r
    poly = jnp.full_like(s, SIN_PI[-1])
    for coef in SIN_PI[-2::-1]:
        poly = poly * s + coef
    half = poly * r
    scale = math.sqrt(2.0 / weights.shape[1])
    return scale - (2.0 * scale) * (half * half)


def packed_slot(block, blocks):
    if block < blocks // 2:
        return block, 0
    return blocks - 1 - block, (block + 1) * NB


def gram_kernel(core, frames, weights, phases, mine, other, high, low):
    quarter = mine.shape[0]
    blocks = quarter * 4
    slabs = jnp.concatenate([frames[i] for i in range(frames.shape[0])], axis=1)
    h, l = split2(features(slabs, weights[...], phases[...]))
    high[...] = h
    low[...] = l
    for i in range(blocks):
        rows = slice(i * NB, (i + 1) * NB)
        right = slice(i * NB, blocks * NB)
        g = dot_t(high[:, rows], high[:, right])
        g = g + dot_t(high[:, rows], low[:, right])
        g = g + dot_t(low[:, rows], high[:, right])
        at, col = packed_slot(i, blocks)
        own = core[0] == at // quarter

        def store(half):
            half[at % quarter, :, col : col + (blocks - i) * NB] = g

        pl.when(own)(lambda: store(mine))
        pl.when(jnp.logical_not(own))(lambda: store(other))


def feature_kernel(order, *refs):
    tops, bottoms, (weights, phases, residual, high, low, corr) = refs[:4], refs[4:8], refs[8:]
    below = pl.program_id(0) >= pl.num_programs(0) // 2
    slabs = [jnp.where(below, b[...], t[...]) for t, b in zip(tops, bottoms)]
    sorted_weights = jnp.concatenate([weights[order[i]] for i in range(4)], axis=0)
    h, l = split2(features(jnp.concatenate(slabs, axis=1), sorted_weights, phases[...]))
    high[...] = h
    low[...] = l
    right = split2(residual[...])
    part = dot3_t((h, l), right)

    @pl.when(pl.program_id(0) == 0)
    def _():
        corr[...] = part

    @pl.when(pl.program_id(0) > 0)
    def _():
        corr[...] += part


def invert_block(d):
    lane = lax.broadcasted_iota(jnp.int32, (PB, NB), 1)
    sub = lax.broadcasted_iota(jnp.int32, (PB, NB), 0)
    col_at = lax.broadcasted_iota(jnp.int32, (NB, NB), 1)
    zero = jnp.zeros((PB, NB), F32)
    for k0 in range(0, NB, PB):
        rows = d[k0 : k0 + PB, :]
        cols = [jnp.broadcast_to(rows[:, k0 + j : k0 + j + 1], (PB, NB)) for j in range(PB)]
        lh, lm, ll = split3(jnp.where(lane < k0, -rows, rows))
        left = jnp.concatenate([lh, lh, lm, lm, lh, ll], axis=0)
        x = jnp.where((lane >= k0) & (lane < k0 + PB), jnp.where(lane - k0 == sub, 1.0, 0.0), rows)
        scale = zero
        for k in range(PB):
            c = cols[k]
            p = 1.0 / c[k : k + 1, :]
            m = jnp.where(sub == k, 0.0, c * p)
            scale = jnp.where(sub == k, p, scale)
            for j in range(k + 1, PB):
                cols[j] = cols[j] - m * cols[j][k : k + 1, :]
            x = x - m * x[k : k + 1, :]
        x = x * scale
        xh, xm, xl = split3(x)
        right = jnp.concatenate([xh, xm, xh, xm, xl, xh], axis=0)
        update = dot_t(left, right)
        kept = d[...]
        d[...] = jnp.where((col_at >= k0) & (col_at < k0 + PB), 0.0, kept) - update
        d[k0 : k0 + PB, :] = x


def factor_steps(rows_of, panel, inverse, left, d, ridge):
    steps, _, width = panel[0].shape
    for ref in (*panel, *left):
        ref[...] = jnp.zeros_like(ref)
    eye = jnp.where(
        lax.broadcasted_iota(jnp.int32, (NB, NB), 0) == lax.broadcasted_iota(jnp.int32, (NB, NB), 1),
        ridge,
        0.0,
    ).astype(F32)

    def step(i, _):
        own = pl.ds(pl.multiple_of(i * NB, NB), NB)
        before = [ref[:, :, own].reshape(steps * NB, NB) for ref in left]
        done = [ref[...].reshape(steps * NB, width) for ref in panel]
        here = [ref[:, :, own].reshape(steps * NB, NB) for ref in panel]
        d[...] = rows_of(i, own) - dot3_t(before, here) + eye
        row = rows_of(i, slice(None)) - dot3_t(before, done)
        parts = split2(row)
        invert_block(d)
        inverse[i] = d[...]
        result = split2(dot(d[...], row, HIGHEST))
        for k in range(2):
            left[k][i] = parts[k]
            panel[k][i] = result[k]
        return 0

    lax.fori_loop(0, steps, step, 0)


def first_factor_kernel(core, mine, other, high, low, inverse, rest, a, lh, ll, d, *, ridge):
    blocks = a.shape[0]
    size = blocks * NB
    quarter = blocks // 4
    steps = high.shape[0]

    def unpack(halves):
        for i in range(blocks):
            at, col = packed_slot(i, blocks)
            a[i, :, i * NB : size] = halves[at // quarter][at % quarter, :, col : col + size - i * NB]

    @pl.when(core[0] == 0)
    def _():
        unpack((mine, other))

    @pl.when(core[0] != 0)
    def _():
        unpack((other, mine))

    for i in range(1, blocks):
        a[i, :, : i * NB] = jnp.zeros((NB, i * NB), F32)
    factor_steps(lambda i, cols: a[i, :, cols], (high, low), inverse, (lh, ll), d, ridge)
    edge = steps * NB
    right = [ref[:, :, edge:].reshape(edge, size - edge) for ref in (high, low)]
    for i in range(steps, blocks):
        cols = slice(i * NB, (i + 1) * NB)
        before = [ref[:, :, cols].reshape(edge, NB) for ref in (lh, ll)]
        rest[i - steps] = a[i, :, edge:] - dot3_t(before, right)


def second_factor_kernel(matrix, high, low, inverse, lh, ll, d, *, ridge):
    factor_steps(lambda i, cols: matrix[i, :, cols], (high, low), inverse, (lh, ll), d, ridge)


def solve_kernel(high0, low0, inverse0, high1, low1, inverse1, corr, out, ch, cl, wh, wl):
    half = high0.shape[0]
    blocks = half + high1.shape[0]
    edge = half * NB

    def store(parts, rows, value):
        for ref, part in zip(parts, split2(value)):
            ref[rows, :] = part

    def known(parts, first, last):
        return [ref[first * NB : last * NB, :] for ref in parts]

    for i in range(blocks):
        rows = slice(i * NB, (i + 1) * NB)
        value = corr[rows, :]
        top = min(i, half)
        if top > 0:
            left = [ref[:top, :, rows].reshape(top * NB, NB) for ref in (high0, low0)]
            value = value - dot3_t(left, known((ch, cl), 0, top))
        if i > half:
            cols = slice(i * NB - edge, (i + 1) * NB - edge)
            left = [ref[: i - half, :, cols].reshape((i - half) * NB, NB) for ref in (high1, low1)]
            value = value - dot3_t(left, known((ch, cl), half, i))
        store((ch, cl), rows, value)
    for i in range(blocks - 1, -1, -1):
        rows = slice(i * NB, (i + 1) * NB)
        inverse = inverse0[i] if i < half else inverse1[i - half]
        value = dot3(split2(inverse), known((ch, cl), i, i + 1))
        if i < blocks - 1:
            panel = (high0, low0) if i < half else (high1, low1)
            base = 0 if i < half else half
            right = [ref[i - base, :, (i + 1 - base) * NB :] for ref in panel]
            value = value - dot3(right, known((wh, wl), i + 1, blocks))
        out[rows, :] = value
        store((wh, wl), rows, value)


def update_kernel(high, low, coef, residual, out):
    wh, wl = split2(coef[...])
    h = high[...]
    out[...] = residual[...] - (dot(h, wh) + dot(h, wl) + dot(low[...], wh))


def cost(us):
    return pl.CostEstimate(flops=int(us * 5e8), bytes_accessed=0, transcendentals=0)


def params(mib, **kw):
    return pltpu.CompilerParams(vmem_limit_bytes=mib * 1024 * 1024, **kw)


def factor_shapes(steps, blocks):
    return (
        jax.ShapeDtypeStruct((steps, NB, blocks * NB), BF16),
        jax.ShapeDtypeStruct((steps, NB, blocks * NB), BF16),
        jax.ShapeDtypeStruct((steps, NB, NB), F32),
    )


def factor_scratch(steps, blocks):
    return [
        pltpu.VMEM((steps, NB, blocks * NB), BF16),
        pltpu.VMEM((steps, NB, blocks * NB), BF16),
        pltpu.VMEM((NB, NB), F32),
    ]


def first_factor_call(core, mine, other, ridge):
    blocks = mine.shape[0] * 4
    steps = blocks // 2
    vmem = pl.BlockSpec(memory_space=pltpu.VMEM)
    return pl.pallas_call(
        lambda *refs: first_factor_kernel(*refs, ridge=ridge),
        in_specs=[pl.BlockSpec(memory_space=pltpu.SMEM), vmem, vmem],
        out_shape=(
            *factor_shapes(steps, blocks),
            jax.ShapeDtypeStruct((blocks - steps, NB, (blocks - steps) * NB), F32),
        ),
        scratch_shapes=[
            pltpu.VMEM((blocks, NB, blocks * NB), F32),
            *factor_scratch(steps, blocks),
        ],
        compiler_params=params(56),
        cost_estimate=cost(28),
        name="factor0",
    )(core, mine, other)


def second_factor_call(matrix, ridge):
    blocks = matrix.shape[0]
    return pl.pallas_call(
        lambda *refs: second_factor_kernel(*refs, ridge=ridge),
        out_shape=factor_shapes(blocks, blocks),
        scratch_shapes=factor_scratch(blocks, blocks),
        compiler_params=params(56),
        cost_estimate=cost(22),
        name="factor1",
    )(matrix)


def solve_call(factors, corr):
    return pl.pallas_call(
        solve_kernel,
        out_shape=jax.ShapeDtypeStruct(corr.shape, F32),
        scratch_shapes=[pltpu.VMEM(corr.shape, BF16) for _ in range(4)],
        compiler_params=params(28),
        cost_estimate=cost(12),
        name="solve",
    )(*factors, corr)


def gram_call(core, frames, weights, phases):
    rows = frames.shape[1]
    feat = weights.shape[1]
    vmem = pl.BlockSpec(memory_space=pltpu.VMEM)
    half = jax.ShapeDtypeStruct((feat // NB // 4, NB, feat + NB), F32)
    return pl.pallas_call(
        gram_kernel,
        in_specs=[pl.BlockSpec(memory_space=pltpu.SMEM), vmem, vmem, vmem],
        out_shape=(half, half),
        scratch_shapes=[pltpu.VMEM((rows, feat), BF16), pltpu.VMEM((rows, feat), BF16)],
        compiler_params=params(28),
        cost_estimate=cost(7),
        name="gram",
    )(core, frames, weights, phases)


def feature_call(order, tops, bottoms, weights, phases, residual, tile=512):
    rows, cols = residual.shape
    width = tops[0].shape[1]
    feat = weights.shape[1]
    half = rows // tile // 2
    return pl.pallas_call(
        feature_kernel,
        grid=(rows // tile,),
        in_specs=[
            pl.BlockSpec(memory_space=pltpu.SMEM),
            *[pl.BlockSpec((tile, width), lambda i: (jnp.minimum(i, half - 1), 0))] * 4,
            *[pl.BlockSpec((tile, width), lambda i: (jnp.maximum(i - half, 0), 0))] * 4,
            pl.BlockSpec((4, width, feat), lambda i: (0, 0, 0)),
            pl.BlockSpec((1, feat), lambda i: (0, 0)),
            pl.BlockSpec((tile, cols), lambda i: (i, 0)),
        ],
        out_specs=[
            pl.BlockSpec((tile, feat), lambda i: (i, 0)),
            pl.BlockSpec((tile, feat), lambda i: (i, 0)),
            pl.BlockSpec((feat, cols), lambda i: (0, 0)),
        ],
        out_shape=[
            jax.ShapeDtypeStruct((rows, feat), BF16),
            jax.ShapeDtypeStruct((rows, feat), BF16),
            jax.ShapeDtypeStruct((feat, cols), F32),
        ],
        compiler_params=params(56, dimension_semantics=("arbitrary",)),
        cost_estimate=cost(15),
        name="features",
    )(order, *tops, *bottoms, weights.reshape(4, width, feat), phases, residual)


def update_call(high, low, coef, residual, tile=256):
    rows, feat = high.shape
    cols = residual.shape[1]
    return pl.pallas_call(
        update_kernel,
        grid=(rows // tile,),
        in_specs=[
            pl.BlockSpec((tile, feat), lambda i: (i, 0)),
            pl.BlockSpec((tile, feat), lambda i: (i, 0)),
            pl.BlockSpec((feat, cols), lambda i: (0, 0)),
            pl.BlockSpec((tile, cols), lambda i: (i, 0)),
        ],
        out_specs=pl.BlockSpec((tile, cols), lambda i: (i, 0)),
        out_shape=jax.ShapeDtypeStruct((rows, cols), F32),
        compiler_params=params(28, dimension_semantics=("arbitrary",)),
        cost_estimate=cost(10),
        name="update",
    )(high, low, coef, residual)


UP = [(i, (i + 1) % 4) for i in range(4)]
DOWN = [(i, (i - 1) % 4) for i in range(4)]
SWAP = [(0, 1), (1, 0)]


def exchange(parts, axes):
    return lax.all_to_all(parts, axes, 0, 0, tiled=True)


def to_everyone(value, axes):
    return exchange(jnp.broadcast_to(value[None], (lax.axis_size(axes), *value.shape)), axes)


def ring_slabs(own):
    half = own.shape[0] // 2
    top, bottom = own[:half], own[half:]
    left_top = lax.ppermute(top, "tgt", UP)
    right_bottom = lax.ppermute(bottom, "tgt", DOWN)
    left_bottom = lax.ppermute(bottom, "tgt", UP)
    right_top = lax.ppermute(top, "tgt", DOWN)
    far_top = lax.ppermute(left_top, "tgt", UP)
    far_bottom = lax.ppermute(right_bottom, "tgt", DOWN)
    return (top, left_top, right_top, far_top), (bottom, left_bottom, right_bottom, far_bottom)


def summed_gram(mine, other):
    other = lax.ppermute(other, "core", SWAP)
    mine = mine + other
    chips = ("y", "z", "tgt")
    count = lax.axis_size(chips)
    parts = mine.reshape(count, -1, mine.shape[-1])
    parts = exchange(parts, chips)
    piece = jnp.sum(parts, axis=0)
    mine = to_everyone(piece, chips).reshape(mine.shape)
    return mine, lax.ppermute(mine, "core", SWAP)


def summed_corr(corr):
    plane = ("y", "z")
    count = lax.axis_size(plane)
    parts = exchange(corr.reshape(count, -1, corr.shape[-1]), plane)
    piece = jnp.sum(parts, axis=0)
    piece = piece + lax.ppermute(piece, "core", SWAP)
    return to_everyone(piece, plane).reshape(corr.shape)


def block_step(frames, weights, phases, residual):
    rows_here = frames.shape[0]
    feature_count = weights.shape[1]
    ridge = 0.1 * rows_here * lax.axis_size(("y", "z", "core")) / feature_count
    phases = phases[None, :]
    core = lax.axis_index("core")
    at = lax.axis_index("tgt")
    whole_rows = exchange(frames.reshape(4, rows_here // 4, -1), "tgt")
    order = jnp.stack([at, at + 3, at + 1, at + 2]) % 4
    tops, bottoms = ring_slabs(frames)
    halves = gram_call(core[None], whole_rows, weights, phases)
    mine, other = summed_gram(*halves)
    high, low, corr = feature_call(order, tops, bottoms, weights, phases, residual)
    corr = summed_corr(corr)
    *factor0, rest = first_factor_call(core[None], mine, other, ridge)
    factor1 = second_factor_call(rest, ridge)
    coefficients = solve_call((*factor0, *factor1), corr)
    residual_next = update_call(high, low, coefficients, residual)
    return (residual_next, coefficients)


def solution(mesh):
    rows = ("y", "z", "core")
    mesh = jax.sharding.Mesh(mesh.devices.reshape(4, 4, 2, 4), (*rows, "tgt"))
    return jax.shard_map(
        block_step,
        mesh=mesh,
        in_specs=(P(rows, "tgt"), P(), P(), P(rows, "tgt")),
        out_specs=(P(rows, "tgt"), P(None, "tgt")),
        check_vma=False,
    )
```
